32 devices in a mesh: row: 8 (over z, core), col: 4 (over y, x).
Axes of the slice: x: 2, y: 2, z: 4, core: 2. Of those that a mesh axis runs over, the one named last changes fastest.
Arguments:
- factor: bfloat16 [8192, 8192], P('row', 'col'), as said below
- sel_tiles: int32 [32], replicated, may hold values from 0 to 63, as said below
- coupling: bfloat16 [8192, 2048], P('col', 'row')
Outputs:
- root_inverse: float32 [8192, 8192], P('row', 'col')
- child_inverse: float32 [2048, 8192], P('col', 'row')
The draws below stay inside these ranges and needn't reach their ends.
Inputs may be any that keep to these rules, and one draw needn't show every extreme that they name: sel_tiles holds 32 distinct tile indices in increasing order; rows of coupling outside the listed tiles are zero. factor is lower triangular with a diagonal between 1 and 1.5.
All inputs are finite; a program needn't handle non-finite values.
Results may differ from the reference program's by a relative error of at most 0.003.
Values may be sent and summed in bfloat16 or wider, within the bound.
A program may use at most 128 MiB of HBM per device.

```python
import jax
import jax.numpy as jnp

S = 8192
TILE = 128
NCH = 2048
R = 32


def chosen_tiles(key):
    order = jax.random.permutation(jax.random.fold_in(key, 7), S // TILE)
    return jnp.sort(order[:R]).astype(jnp.int32)


def draw_sel_tiles(key, part):
    return chosen_tiles(key)


def draw_factor(key, part):
    first = jax.random.fold_in(key, 11)
    second = jax.random.fold_in(key, 13)
    rows = jnp.arange(S)[:, None]
    cols = jnp.arange(S)[None, :]
    lower = jax.random.normal(first, (S, S), jnp.float32)
    lower = lower * S ** (-0.5)
    diag = 1.0 + 0.5 * jax.random.uniform(second, (S,), jnp.float32)
    full = jnp.where(rows > cols, lower, 0.0) + jnp.where(rows == cols, diag[None, :], 0.0)
    return full.astype(jnp.bfloat16)


def draw_coupling(key, part):
    tiles = chosen_tiles(key)
    tile_of = (jnp.arange(S) // TILE).astype(jnp.int32)
    member = jnp.any(tile_of[:, None] == tiles[None, :], axis=1)
    values = 0.5 * jax.random.normal(jax.random.fold_in(key, 5), (S, NCH), jnp.float32)
    return jnp.where(member[:, None], values, 0.0).astype(jnp.bfloat16)


def setup_inputs(seed: int = 0) -> dict:
    key_of = jax.random.split(jax.random.key(seed), 4)
    factor = draw_factor(jax.random.fold_in(key_of[3], 71), 0)
    sel_tiles = draw_sel_tiles(jax.random.fold_in(key_of[3], 71), 0)
    coupling = draw_coupling(jax.random.fold_in(key_of[3], 71), 0)
    return {"factor": factor, "sel_tiles": sel_tiles, "coupling": coupling}


def reference(factor, sel_tiles, coupling):
    gram = jnp.dot(factor.T, factor, preferred_element_type=jnp.float32)
    rounded = gram.astype(jnp.bfloat16)
    tile_of = (jnp.arange(S) // TILE).astype(jnp.int32)
    member = jnp.any(tile_of[:, None] == sel_tiles[None, :], axis=1)
    product = jnp.dot(coupling.T, rounded.T, preferred_element_type=jnp.float32)
    child = jnp.where(member[None, :], -product, jnp.float32(0.0))
    return gram, child
```

```python
import functools
import math

import jax
import jax.numpy as jnp
from jax import lax
from jax.experimental import pallas as pl
from jax.experimental.pallas import tpu as pltpu
from jax.sharding import PartitionSpec as P

TILE = 128
MESH = pl.DeviceIdType.MESH
SKEW = 2


def gather_kernel(dims, f_ref, a_ref, b_ref, recv_a, recv_b, send_z, send_p, send_b, send_f, local_a, local_b):
    levels, wide, high, cores, chunks = dims
    rows, width = f_ref.shape
    narrow = width // cores
    h = rows // chunks
    r, c = lax.axis_index("row"), lax.axis_index("col")
    k, z = lax.rem(r, cores), r // cores
    x, y = lax.rem(c, wide), c // wide
    x0, y0 = lax.rem(z, wide), z // wide
    source = c == z

    def chunk_rows(block, j):
        return pl.ds(pl.multiple_of(block * rows + j * h, h), h)

    def remote(src, dst, send, recv, row, col):
        return pltpu.make_async_remote_copy(
            src_ref=src, dst_ref=dst, send_sem=send, recv_sem=recv,
            device_id=(row, col), device_id_type=MESH,
        )

    def copies(t, j):
        m = z + t
        inside = m < levels
        has = inside & (m >= c)
        block = m * cores + k
        at = chunk_rows(block, j)
        if t == 0:
            def src(cols):
                return f_ref.at[pl.ds(j * h, h), cols]
        else:
            def src(cols):
                return a_ref.at[at, cols]
        everything = pl.ds(0, width)
        found = []
        for kk in range(cores):
            piece = src(pl.ds(kk * narrow, narrow))
            into = b_ref.at[at, :]
            for dx in range(1, wide):
                xt = lax.rem(x + dx, wide)
                found.append((
                    source & inside & (m >= y * wide + xt),
                    remote(piece, into, send_b.at[kk, dx, t, j], recv_b.at[block, j],
                           z * cores + kk, y * wide + xt),
                    False,
                ))
            for dy in range(1, high):
                yt = lax.rem(y + dy, high)
                found.append((
                    source & inside & (m >= yt * wide),
                    remote(piece, into, send_b.at[kk, wide - 1 + dy, t, j], recv_b.at[block, j],
                           z * cores + kk, yt * wide + x),
                    False,
                ))
        found.append((
            has & (z > 0),
            remote(src(everything), a_ref.at[at, :], send_z.at[t, j], recv_a.at[block, j],
                   r - cores, c),
            False,
        ))
        for dk in range(1, cores):
            other = z * cores + lax.rem(k + dk, cores)
            found.append((
                has,
                remote(src(everything), a_ref.at[at, :], send_p.at[dk, t, j], recv_a.at[block, j], other, c),
                False,
            ))
        for kk in range(cores):
            piece = src(pl.ds(kk * narrow, narrow))
            into = b_ref.at[at, :]
            found.append((
                source & inside & (k != kk),
                remote(piece, into, send_b.at[kk, 0, t, j], recv_b.at[block, j], z * cores + kk, c),
                False,
            ))
            found.append((
                source & inside & (k == kk),
                pltpu.make_async_copy(piece, into, local_b.at[t, j]),
                True,
            ))
        if t == 0:
            found.append((has, pltpu.make_async_copy(src(everything), a_ref.at[at, :], local_a.at[j]), True))
        return found

    def forwards(t, j, p):
        m = z + t
        block = m * cores + p
        part = b_ref.at[chunk_rows(block, j), :]
        mine = (x == x0) & (y != y0) & (m < levels)
        found = []
        for dx in range(1, wide):
            xt = lax.rem(x + dx, wide)
            found.append((
                mine & (m >= y * wide + xt),
                remote(part, part, send_f.at[dx, p, t, j], recv_b.at[block, j], r, y * wide + xt),
            ))
        return mine & (m >= y * wide), found

    def arrived(ref, sem):
        remote(ref, ref, send_z.at[0, 0], sem, r, c).wait_recv()

    def step(t, j):
        m = z + t
        block = m * cores + k
        if t > 0:
            @pl.when((m < levels) & (m >= c))
            def _():
                arrived(a_ref.at[chunk_rows(block, j), :], recv_a.at[block, j])
        for condition, copy, _ in copies(t, j):
            pl.when(condition)(copy.start)

    def forward(t, j):
        for p in range(cores):
            due, found = forwards(t, j, p)
            block = (z + t) * cores + p

            @pl.when(due)
            def _():
                arrived(b_ref.at[chunk_rows(block, j), :], recv_b.at[block, j])
            for condition, copy in found:
                pl.when(condition)(copy.start)

    order = [(t, j) for t in range(levels) for j in range(chunks)]
    for n, (t, j) in enumerate(order):
        step(t, j)
        if n >= SKEW:
            forward(*order[n - SKEW])
    for t, j in order[len(order) - SKEW:]:
        forward(t, j)

    for t, j in order:
        m = z + t
        inside = m < levels
        for dk in range(1, cores):
            block = m * cores + lax.rem(k + dk, cores)

            @pl.when(inside & (m >= c))
            def _():
                arrived(a_ref.at[chunk_rows(block, j), :], recv_a.at[block, j])

            @pl.when(inside & source)
            def _():
                arrived(b_ref.at[chunk_rows(block, j), :], recv_b.at[block, j])
        for p in range(cores):
            block = m * cores + p

            @pl.when(inside & (x != x0) & (m >= c))
            def _():
                arrived(b_ref.at[chunk_rows(block, j), :], recv_b.at[block, j])
        for condition, copy, local in copies(t, j):
            pl.when(condition)(copy.wait if local else copy.wait_send)
        for p in range(cores):
            for condition, copy in forwards(t, j, p)[1]:
                pl.when(condition)(copy.wait_send)


def gather(factor, n_row, n_col):
    rows, width = factor.shape
    cores = n_row // n_col
    wide = next(w for w in range(math.isqrt(n_col), 0, -1) if n_col % w == 0)
    high = n_col // wide
    levels = n_col
    chunks = max(1, 32 // n_row)
    dma = pltpu.SemaphoreType.DMA
    whole = rows * n_row
    return pl.pallas_call(
        functools.partial(gather_kernel, (levels, wide, high, cores, chunks)),
        out_shape=(
            jax.ShapeDtypeStruct((whole, width), factor.dtype),
            jax.ShapeDtypeStruct((whole, width // cores), factor.dtype),
        ),
        in_specs=[pl.BlockSpec(memory_space=pl.ANY)],
        out_specs=(pl.BlockSpec(memory_space=pl.ANY), pl.BlockSpec(memory_space=pl.ANY)),
        scratch_shapes=[
            dma((n_row, chunks)),
            dma((n_row, chunks)),
            dma((levels, chunks)),
            dma((cores, levels, chunks)),
            dma((cores, wide + high, levels, chunks)),
            dma((wide, cores, levels, chunks)),
            dma((chunks,)),
            dma((levels, chunks)),
        ],
        compiler_params=pltpu.CompilerParams(has_side_effects=True),
        cost_estimate=pl.CostEstimate(flops=0, bytes_accessed=whole * width * 32, transcendentals=0),
    )(factor)


def exchange_kernel(n_col, part_ref, out_ref, send, recv):
    r, c = lax.axis_index("row"), lax.axis_index("col")
    depth = out_ref.shape[1]
    started = []
    for d in range(1, n_col):
        ct = lax.rem(c + d, n_col)
        copy = pltpu.make_async_remote_copy(
            src_ref=part_ref.at[pl.ds(pl.multiple_of(ct * depth, depth), depth), :],
            dst_ref=out_ref.at[d - 1],
            send_sem=send.at[d - 1],
            recv_sem=recv.at[d - 1],
            device_id=(r, ct),
            device_id_type=MESH,
        )
        copy.start()
        started.append(copy)
    for copy in started:
        copy.wait()


def exchange(part, n_col):
    total, width = part.shape
    dma = pltpu.SemaphoreType.DMA
    return pl.pallas_call(
        functools.partial(exchange_kernel, n_col),
        out_shape=jax.ShapeDtypeStruct((n_col - 1, total // n_col, width), part.dtype),
        in_specs=[pl.BlockSpec(memory_space=pl.ANY)],
        out_specs=pl.BlockSpec(memory_space=pl.ANY),
        scratch_shapes=[dma((n_col - 1,)), dma((n_col - 1,))],
        compiler_params=pltpu.CompilerParams(has_side_effects=True),
    )(part)


def body(n_row, n_col, factor, sel_tiles, coupling):
    rows_here = factor.shape[0]
    row_index, col_index = lax.axis_index("row"), lax.axis_index("col")
    cores = n_row // n_col
    below, partner = gather(factor, n_row, n_col)
    coupling_full = lax.all_gather(coupling, "row", axis=1, tiled=True)

    def product(level, below, partner):
        first = level * rows_here * cores
        return lax.dot_general(
            partner[first:], below[first:], (((0,), (0,)), ((), ())), preferred_element_type=jnp.float32
        )

    gram = lax.switch(
        jnp.maximum(row_index // cores, col_index),
        [functools.partial(product, level) for level in range(n_col)],
        below,
        partner,
    )
    rounded = gram.astype(jnp.bfloat16)
    global_rows = row_index * rows_here + jnp.arange(rows_here, dtype=jnp.int32)
    member = jnp.any((global_rows // TILE)[:, None] == sel_tiles[None, :], axis=1)
    part = lax.dot_general(
        coupling_full, rounded, (((0,), (1,)), ((), ())), preferred_element_type=jnp.float32
    ).astype(jnp.bfloat16)
    depth = part.shape[0] // n_col
    arrived = exchange(part, n_col)
    summed = lax.dynamic_slice_in_dim(part, col_index * depth, depth, 0).astype(jnp.float32)
    for d in range(n_col - 1):
        summed = summed + arrived[d].astype(jnp.float32)
    child = jnp.where(member[None, :], -summed, jnp.float32(0.0))
    return (gram, child)


def solution(mesh):
    placed = (P("row", "col"), P(), P("col", "row"))
    return jax.shard_map(
        functools.partial(body, mesh.shape["row"], mesh.shape["col"]),
        mesh=mesh,
        in_specs=placed,
        out_specs=(P("row", "col"), P("col", "row")),
        check_vma=False,
    )
```

```python
import functools
import math

import jax
import jax.numpy as jnp
from jax import lax
from jax.experimental import pallas as pl
from jax.experimental.pallas import tpu as pltpu
from jax.sharding import PartitionSpec as P

TILE = 128
MESH = pl.DeviceIdType.MESH
SKEW = 2


def gather_kernel(dims, f_ref, a_ref, b_ref, recv_a, recv_b, send_z, send_p, send_b, send_f, local_a, stage):
    levels, wide, high, cores, chunks = dims
    rows, width = f_ref.shape
    narrow = width // cores
    h = rows // chunks
    r, c = lax.axis_index("row"), lax.axis_index("col")
    k, z = lax.rem(r, cores), r // cores
    x, y = lax.rem(c, wide), c // wide
    x0, y0 = lax.rem(z, wide), z // wide
    source = c == z

    def chunk_rows(block, j):
        return pl.ds(pl.multiple_of(block * rows + j * h, h), h)

    def remote(src, dst, send, recv, row, col):
        return pltpu.make_async_remote_copy(
            src_ref=src, dst_ref=dst, send_sem=send, recv_sem=recv,
            device_id=(row, col), device_id_type=MESH,
        )

    def copies(t, j):
        m = z + t
        inside = m < levels
        has = inside & (m >= c)
        block = m * cores + k
        at = chunk_rows(block, j)
        if t == 0:
            def src(cols):
                return f_ref.at[pl.ds(j * h, h), cols]
        else:
            def src(cols):
                return a_ref.at[at, cols]
        everything = pl.ds(0, width)
        found = []
        for kk in range(cores):
            piece = src(pl.ds(kk * narrow, narrow))
            into = b_ref.at[at, :]
            for dx in range(1, wide):
                xt = lax.rem(x + dx, wide)
                found.append((
                    source & inside & (m >= y * wide + xt),
                    remote(piece, into, send_b.at[kk, dx, t, j], recv_b.at[block, j],
                           z * cores + kk, y * wide + xt),
                    False,
                ))
            for dy in range(1, high):
                yt = lax.rem(y + dy, high)
                found.append((
                    source & inside & (m >= yt * wide),
                    remote(piece, into, send_b.at[kk, wide - 1 + dy, t, j], recv_b.at[block, j],
                           z * cores + kk, yt * wide + x),
                    False,
                ))
        found.append((
            has & (z > 0),
            remote(src(everything), a_ref.at[at, :], send_z.at[t, j], recv_a.at[block, j],
                   r - cores, c),
            False,
        ))
        for dk in range(1, cores):
            other = z * cores + lax.rem(k + dk, cores)
            found.append((
                has,
                remote(src(everything), a_ref.at[at, :], send_p.at[dk, t, j], recv_a.at[block, j], other, c),
                False,
            ))
        for kk in range(cores):
            piece = src(pl.ds(kk * narrow, narrow))
            into = b_ref.at[at, :]
            found.append((
                source & inside & (k != kk),
                remote(piece, into, send_b.at[kk, 0, t, j], recv_b.at[block, j], z * cores + kk, c),
                False,
            ))
        return found

    def keep(t, j):
        m = z + t
        at = chunk_rows(m * cores + k, j)
        here = f_ref.at[pl.ds(j * h, h), :] if t == 0 else a_ref.at[at, :]
        inside = (m < levels) & (m >= c)

        @pl.when(inside if t == 0 else inside & source)
        def _():
            load = pltpu.make_async_copy(here, stage, local_a.at[0])
            load.start()
            load.wait()
            if t == 0:
                pltpu.make_async_copy(stage, a_ref.at[at, :], local_a.at[1]).start()
            for kk in range(cores):
                @pl.when(source & (k == kk))
                def _():
                    store = pltpu.make_async_copy(
                        stage.at[:, pl.ds(kk * narrow, narrow)], b_ref.at[at, :], local_a.at[2]
                    )
                    store.start()
                    store.wait()
            if t == 0:
                pltpu.make_async_copy(stage, a_ref.at[at, :], local_a.at[1]).wait()

    def forwards(t, j, p):
        m = z + t
        block = m * cores + p
        part = b_ref.at[chunk_rows(block, j), :]
        mine = (x == x0) & (y != y0) & (m < levels)
        found = []
        for dx in range(1, wide):
            xt = lax.rem(x + dx, wide)
            found.append((
                mine & (m >= y * wide + xt),
                remote(part, part, send_f.at[dx, p, t, j], recv_b.at[block, j], r, y * wide + xt),
            ))
        return mine & (m >= y * wide), found

    def arrived(ref, sem):
        remote(ref, ref, send_z.at[0, 0], sem, r, c).wait_recv()

    def step(t, j):
        m = z + t
        block = m * cores + k
        if t > 0:
            @pl.when((m < levels) & (m >= c))
            def _():
                arrived(a_ref.at[chunk_rows(block, j), :], recv_a.at[block, j])
        for condition, copy, _ in copies(t, j):
            pl.when(condition)(copy.start)
        keep(t, j)

    def forward(t, j):
        for p in range(cores):
            due, found = forwards(t, j, p)
            block = (z + t) * cores + p

            @pl.when(due)
            def _():
                arrived(b_ref.at[chunk_rows(block, j), :], recv_b.at[block, j])
            for condition, copy in found:
                pl.when(condition)(copy.start)

    order = [(t, j) for t in range(levels) for j in range(chunks)]
    for n, (t, j) in enumerate(order):
        step(t, j)
        if n >= SKEW:
            forward(*order[n - SKEW])
    for t, j in order[len(order) - SKEW:]:
        forward(t, j)

    for t, j in order:
        m = z + t
        inside = m < levels
        for dk in range(1, cores):
            block = m * cores + lax.rem(k + dk, cores)

            @pl.when(inside & (m >= c))
            def _():
                arrived(a_ref.at[chunk_rows(block, j), :], recv_a.at[block, j])

            @pl.when(inside & source)
            def _():
                arrived(b_ref.at[chunk_rows(block, j), :], recv_b.at[block, j])
        for p in range(cores):
            block = m * cores + p

            @pl.when(inside & (x != x0) & (m >= c))
            def _():
                arrived(b_ref.at[chunk_rows(block, j), :], recv_b.at[block, j])
        for condition, copy, local in copies(t, j):
            pl.when(condition)(copy.wait if local else copy.wait_send)
        for p in range(cores):
            for condition, copy in forwards(t, j, p)[1]:
                pl.when(condition)(copy.wait_send)


def gather(factor, n_row, n_col):
    rows, width = factor.shape
    cores = n_row // n_col
    wide = next(w for w in range(math.isqrt(n_col), 0, -1) if n_col % w == 0)
    high = n_col // wide
    levels = n_col
    chunks = max(1, 32 // n_row)
    dma = pltpu.SemaphoreType.DMA
    whole = rows * n_row
    return pl.pallas_call(
        functools.partial(gather_kernel, (levels, wide, high, cores, chunks)),
        out_shape=(
            jax.ShapeDtypeStruct((whole, width), factor.dtype),
            jax.ShapeDtypeStruct((whole, width // cores), factor.dtype),
        ),
        in_specs=[pl.BlockSpec(memory_space=pl.ANY)],
        out_specs=(pl.BlockSpec(memory_space=pl.ANY), pl.BlockSpec(memory_space=pl.ANY)),
        scratch_shapes=[
            dma((n_row, chunks)),
            dma((n_row, chunks)),
            dma((levels, chunks)),
            dma((cores, levels, chunks)),
            dma((cores, wide + high, levels, chunks)),
            dma((wide, cores, levels, chunks)),
            dma((3,)),
            pltpu.VMEM((rows // chunks, width), factor.dtype),
        ],
        compiler_params=pltpu.CompilerParams(has_side_effects=True),
        cost_estimate=pl.CostEstimate(flops=0, bytes_accessed=whole * width * 32, transcendentals=0),
    )(factor)


def exchange_kernel(n_col, part_ref, out_ref, send, recv):
    r, c = lax.axis_index("row"), lax.axis_index("col")
    depth = out_ref.shape[1]
    started = []
    for d in range(1, n_col):
        ct = lax.rem(c + d, n_col)
        copy = pltpu.make_async_remote_copy(
            src_ref=part_ref.at[pl.ds(pl.multiple_of(ct * depth, depth), depth), :],
            dst_ref=out_ref.at[d - 1],
            send_sem=send.at[d - 1],
            recv_sem=recv.at[d - 1],
            device_id=(r, ct),
            device_id_type=MESH,
        )
        copy.start()
        started.append(copy)
    for copy in started:
        copy.wait()


def exchange(part, n_col):
    total, width = part.shape
    dma = pltpu.SemaphoreType.DMA
    return pl.pallas_call(
        functools.partial(exchange_kernel, n_col),
        out_shape=jax.ShapeDtypeStruct((n_col - 1, total // n_col, width), part.dtype),
        in_specs=[pl.BlockSpec(memory_space=pl.ANY)],
        out_specs=pl.BlockSpec(memory_space=pl.ANY),
        scratch_shapes=[dma((n_col - 1,)), dma((n_col - 1,))],
        compiler_params=pltpu.CompilerParams(has_side_effects=True),
    )(part)


def body(n_row, n_col, factor, sel_tiles, coupling):
    rows_here = factor.shape[0]
    row_index, col_index = lax.axis_index("row"), lax.axis_index("col")
    cores = n_row // n_col
    below, partner = gather(factor, n_row, n_col)
    coupling_full = lax.all_gather(coupling, "row", axis=1, tiled=True)

    def product(level, below, partner):
        first = level * rows_here * cores
        return lax.dot_general(
            partner[first:], below[first:], (((0,), (0,)), ((), ())), preferred_element_type=jnp.float32
        )

    gram = lax.switch(
        jnp.maximum(row_index // cores, col_index),
        [functools.partial(product, level) for level in range(n_col)],
        below,
        partner,
    )
    rounded = gram.astype(jnp.bfloat16)
    global_rows = row_index * rows_here + jnp.arange(rows_here, dtype=jnp.int32)
    member = jnp.any((global_rows // TILE)[:, None] == sel_tiles[None, :], axis=1)
    part = lax.dot_general(
        coupling_full, rounded, (((0,), (1,)), ((), ())), preferred_element_type=jnp.float32
    ).astype(jnp.bfloat16)
    depth = part.shape[0] // n_col
    arrived = exchange(part, n_col)
    summed = lax.dynamic_slice_in_dim(part, col_index * depth, depth, 0).astype(jnp.float32)
    for d in range(n_col - 1):
        summed = summed + arrived[d].astype(jnp.float32)
    child = jnp.where(member[None, :], -summed, jnp.float32(0.0))
    return (gram, child)


def solution(mesh):
    placed = (P("row", "col"), P(), P("col", "row"))
    return jax.shard_map(
        functools.partial(body, mesh.shape["row"], mesh.shape["col"]),
        mesh=mesh,
        in_specs=placed,
        out_specs=(P("row", "col"), P("col", "row")),
        check_vma=False,
    )
```
